32 devices in a mesh: grp: 2 (over y), mode: 8 (over z, x), node: 2 (over core).
Axes of the slice: x: 2, y: 2, z: 4, core: 2. Of those that a mesh axis runs over, the one named last changes fastest.
Arguments:
- mode_basis: float32 [4096, 4096], P('mode', 'node'), may hold values from -6 to 6
- mode_scales: float32 [4096], P('mode'), may hold values from 0.003 to 0.02
- mean_log: float32 [4096], P(('node', 'mode')), may hold values from -0.5 to 0.5
- sample_seeds: int32 [4096], P('grp'), parts along dimension 0, may hold values from 0 to 1073741823
Outputs:
- modulus: float32 [4096, 4096], P(('node', 'mode'), 'grp'), parts along dimension 1
- sample_means: float32 [4096], P('grp'), parts along dimension 0
The draws below stay inside these ranges and needn't reach their ends.
There are 2 independent parts, one for each index of `grp`. The reference program is written for one: setup_inputs(seed, part) draws one part's arguments, and reference() takes and returns one part's arrays. A program takes and returns all parts, laid end to end along the dimension named above; an argument that names none is the same for every part. Nothing has to cross between parts.
All inputs are finite; a program needn't handle non-finite values.
Results may differ from the reference program's by a relative error of at most 0.00005.
Values sent between devices are 32-bit elements; how exact they have to be, the bound alone decides.
No kernel may reach another device: no remote copies, remote signals or barrier semaphores. Data moves between devices by JAX's collectives and lax.ppermute only.
A program may use at most 64 MiB of HBM per device.

```python
import math
import jax
import jax.numpy as jnp
from jax import lax

MODES = 4096
SAMPLES = 2048
NODES = 4096


def plant(entries, own_key, smallest, top_value):
    spot = [jax.random.randint(jax.random.fold_in(own_key, axis), (), 0, length) for axis, length in enumerate(entries.shape)]
    widest = entries.shape.index(max(entries.shape))
    neighbour = spot[:widest] + [(spot[widest] + 1) % entries.shape[widest]] + spot[widest + 1:]
    return entries.at[tuple(spot)].set(smallest).at[tuple(neighbour)].set(top_value)


def with_spikes(array, own_key, source, target, blocks, factor):
    owner, partner = [(jnp.arange(array.shape[axis_at]) // (array.shape[axis_at] // blocks)).reshape([-1 if axis == axis_at else 1 for axis in range(array.ndim)]) for axis_at in (source, target)]
    chosen = jax.random.permutation(own_key, blocks)[partner]
    strong = (owner == chosen) | (owner == (partner + blocks // 2) % blocks)
    return jnp.where(strong, factor * array, array)


def level_of(stream_key, dims, split, low, high):
    loudness, own = 1.0, jax.random.fold_in(stream_key, 6)
    for axis_at, shards_of in split:
        draws = jnp.exp(jax.random.uniform(jax.random.fold_in(own, axis_at), (shards_of,), jnp.float32, low / len(split), high / len(split)))
        loudness = loudness * jnp.repeat(draws, dims[axis_at] // shards_of).reshape([-1 if axis == axis_at else 1 for axis in range(len(dims))])
    return loudness


def bell_draw_with(rng, shape, spread, reach, pieces, heavy, kind=jnp.bfloat16):
    entries = spread * jax.random.normal(rng, shape, jnp.float32)
    if pieces:
        entries = entries * level_of(rng, shape, pieces, -0.22, 0.18)
    return jnp.clip(with_spikes(entries, jax.random.fold_in(rng, 3), *heavy), -reach, reach).astype(kind)


def setup_inputs(seed: int = 0, part: int = 0) -> dict:
    key_of = jax.random.split(jax.random.key(seed), 5)
    own_keys = jax.random.split(jax.random.fold_in(key_of[4], part), 5)
    return {
        "mode_basis": bell_draw_with(key_of[0], (MODES, NODES), 1.0, 6.0, ((0, 8), (1, 2)), (0, 1, 8, 2.0), jnp.float32),
        "mode_scales": jnp.clip(jnp.exp(math.log(0.02) - 1.89712 * jax.random.uniform(key_of[1], (MODES,), jnp.float32) ** level_of(key_of[1], (MODES,), ((0, 8),), -0.2, 0.2)), 0.003, 0.02),
        "mean_log": jnp.clip(jax.random.uniform(key_of[2], (NODES,), jnp.float32, -0.5, 0.5) * level_of(key_of[2], (NODES,), ((0, 16),), -0.4, 0.0), -0.5, 0.5),
        "sample_seeds": plant(jax.random.randint(own_keys[3], (SAMPLES,), 0, 1073741824), jax.random.fold_in(own_keys[3], 1), 0, 1073741823).astype(jnp.int32),
    }


def scramble(seed_words, counter_words):
    mixed_word = seed_words * -1640531527 + counter_words * 668265261
    mixed_word = mixed_word ^ mixed_word >> 15 & 131071
    mixed_word = mixed_word * -2048144789
    mixed_word = mixed_word ^ mixed_word >> 13 & 524287
    mixed_word = mixed_word * -1028477387
    mixed_word = mixed_word ^ mixed_word >> 16 & 65535
    return mixed_word

def normals(sample_seeds, mode_start, mode_count):
    mode_ids = mode_start + jnp.arange(mode_count, dtype=jnp.int32)
    seed_words = sample_seeds.astype(jnp.int32)[None, :]
    counter_words = (2 * mode_ids).astype(jnp.int32)[:, None]
    first_word = scramble(seed_words, counter_words)
    second_word = scramble(seed_words, counter_words + 1)
    first_unit = ((first_word & 16777215).astype(jnp.float32) + 0.5) * (1.0 / 16777216.0)
    second_unit = ((second_word & 16777215).astype(jnp.float32) + 0.5) * (1.0 / 16777216.0)
    radius = jnp.sqrt(-2.0 * jnp.log(first_unit))
    return radius * jnp.cos(2.0 * math.pi * second_unit)

def reference(mode_basis, mode_scales, mean_log, sample_seeds):
    scaled = mode_scales[:, None] * mode_basis
    coeffs = normals(sample_seeds, 0, MODES)
    summed = lax.dot_general(scaled, coeffs, (((0,), (0,)), ((), ())), precision=lax.Precision.HIGHEST, preferred_element_type=jnp.float32)
    modulus = jnp.exp(mean_log[:, None] + summed)
    sample_means = lax.optimization_barrier(jnp.sum(modulus, axis=0)) / NODES
    return (modulus, sample_means)
```

```python
import functools

import jax
import jax.numpy as jnp
from jax import lax
from jax.experimental import pallas as pl
from jax.experimental.pallas import tpu as pltpu
from jax.sharding import PartitionSpec as P

SEED_FACTOR = -1640531527
COUNT_FACTOR = 668265261
COS_TERMS = (1.4142134962552295, -6.97885094856384, 5.73946037690727, -1.8835579059862844, 0.31068802752475627)
SUB = 16


def scramble(word):
    word = word ^ lax.shift_right_logical(word, 15)
    word = word * -2048144789
    word = word ^ lax.shift_right_logical(word, 13)
    word = word * -1028477387
    return word ^ lax.shift_right_logical(word, 16)


def normals(first):
    one = scramble(first) & 16777215
    two = scramble(first + COUNT_FACTOR) << 8
    first_unit = one.astype(jnp.float32) * (1.0 / 16777216.0) + (0.5 / 16777216.0)
    turn = two.astype(jnp.float32) * (2.0**-32) + (0.5 / 16777216.0)
    square = jnp.maximum(-2.0 * jnp.log(first_unit), 1e-30)
    radius = square * lax.rsqrt(square)
    arg = turn * turn
    half = jnp.float32(COS_TERMS[-1])
    for term in COS_TERMS[-2::-1]:
        half = half * arg + jnp.float32(term)
    return radius * (half * half - 1.0)


def split(values):
    high = values.astype(jnp.bfloat16)
    return high, (values - high.astype(jnp.float32)).astype(jnp.bfloat16)


def fill_rows(seeds_ref, high_ref, low_ref, first_mode, rows):
    samples = seeds_ref.shape[1]
    row_terms = lax.broadcasted_iota(jnp.int32, (SUB, 128), 0) * (2 * COUNT_FACTOR % 2**32 - (2**32 if 2 * COUNT_FACTOR % 2**32 >= 2**31 else 0))

    def group(i, carry):
        start = pl.multiple_of(i * SUB, SUB)
        mode_terms = row_terms + (first_mode + start) * 2 * COUNT_FACTOR
        for at in range(0, samples, 128):
            first = seeds_ref[:, at:at + 128] * SEED_FACTOR + mode_terms
            high, low = split(normals(first))
            high_ref[pl.ds(start, SUB), at:at + 128] = high
            low_ref[pl.ds(start, SUB), at:at + 128] = low
        return carry

    lax.fori_loop(0, rows // SUB, group, 0)


def draw_kernel(rows, seeds_ref, high_ref, low_ref):
    fill_rows(seeds_ref, high_ref, low_ref, pl.program_id(0) * rows, rows)


def draw(seeds, modes):
    rows = 256
    samples = seeds.shape[1]
    out = jax.ShapeDtypeStruct((modes, samples), jnp.bfloat16)
    spec = pl.BlockSpec((rows, samples), lambda i: (i, 0))
    return pl.pallas_call(
        functools.partial(draw_kernel, rows),
        grid=(modes // rows,),
        in_specs=[pl.BlockSpec((1, samples), lambda i: (0, 0))],
        out_specs=[spec, spec],
        out_shape=[out, out],
        name="draw",
    )(seeds)


def dot(a, b):
    return lax.dot_general(a, b, (((0,), (0,)), ((), ())), preferred_element_type=jnp.float32)


def contract_kernel(basis_ref, high_ref, low_ref, mean_ref, out_ref, sum_ref):
    step = pl.program_id(0)

    @pl.when(step == 0)
    def _():
        out_ref[...] = jnp.zeros_like(out_ref)

    basis_high, basis_low = split(basis_ref[...])
    out_ref[...] += dot(basis_high, high_ref[...]) + dot(basis_high, low_ref[...]) + dot(basis_low, high_ref[...])

    @pl.when(step == pl.num_programs(0) - 1)
    def _():
        modulus = jnp.exp(out_ref[...] + mean_ref[...])
        out_ref[...] = modulus
        sum_ref[...] = jnp.sum(modulus, axis=0, keepdims=True)


def contract(basis, high, low, mean):
    rows = 512
    modes, nodes = basis.shape
    samples = high.shape[1]
    spec = pl.BlockSpec((rows, samples), lambda i: (i, 0))
    return pl.pallas_call(
        contract_kernel,
        grid=(modes // rows,),
        in_specs=[pl.BlockSpec((rows, nodes), lambda i: (i, 0)), spec, spec, pl.BlockSpec((nodes, 1), lambda i: (0, 0))],
        out_specs=[pl.BlockSpec((nodes, samples), lambda i: (0, 0)), pl.BlockSpec((1, samples), lambda i: (0, 0))],
        out_shape=[jax.ShapeDtypeStruct((nodes, samples), jnp.float32), jax.ShapeDtypeStruct((1, samples), jnp.float32)],
        name="contract",
    )(basis, high, low, mean)


def on_device(mode_basis, mode_scales, mean_log, sample_seeds):
    own_rows = mean_log.shape[0]
    scaled = mode_scales[:, None] * mode_basis
    gathered = lax.all_to_all(scaled, "mode", split_axis=1, concat_axis=0, tiled=True)
    high, low = draw(sample_seeds[None, :], gathered.shape[0])
    modulus, sums = contract(gathered, high, low, mean_log[:, None])
    totals = lax.psum(sums[0], ("mode", "node"))
    node_count = own_rows * lax.axis_size("mode") * lax.axis_size("node")
    return (modulus, totals / node_count)


def solution(mesh):
    return jax.shard_map(
        on_device,
        mesh=mesh,
        in_specs=(P("mode", "node"), P("mode"), P(("node", "mode")), P("grp")),
        out_specs=(P(("node", "mode"), "grp"), P("grp")),
        check_vma=False,
    )
```

```python
import functools

import jax
import jax.numpy as jnp
from jax import lax
from jax.experimental import pallas as pl
from jax.experimental.pallas import tpu as pltpu
from jax.sharding import PartitionSpec as P

SEED_FACTOR = -1640531527
COUNT_FACTOR = 668265261
COS_TERMS = (1.4142134962552295, -6.97885094856384, 5.73946037690727, -1.8835579059862844, 0.31068802752475627)
SUB = 16
DRAW_FLOPS = 8192


def scramble(word):
    word = word ^ lax.shift_right_logical(word, 15)
    word = word * -2048144789
    word = word ^ lax.shift_right_logical(word, 13)
    word = word * -1028477387
    return word ^ lax.shift_right_logical(word, 16)


def normals(first):
    one = scramble(first) & 16777215
    two = scramble(first + COUNT_FACTOR) << 8
    first_unit = one.astype(jnp.float32) * (1.0 / 16777216.0) + (0.5 / 16777216.0)
    turn = two.astype(jnp.float32) * (2.0**-32) + (0.5 / 16777216.0)
    square = jnp.maximum(-2.0 * jnp.log(first_unit), 1e-30)
    radius = square * lax.rsqrt(square)
    arg = turn * turn
    half = jnp.float32(COS_TERMS[-1])
    for term in COS_TERMS[-2::-1]:
        half = half * arg + jnp.float32(term)
    return radius * (half * half - 1.0)


def split(values):
    high = values.astype(jnp.bfloat16)
    return high, (values - high.astype(jnp.float32)).astype(jnp.bfloat16)


def fill_rows(seeds_ref, high_ref, low_ref, first_mode, rows):
    samples = seeds_ref.shape[1]
    row_terms = lax.broadcasted_iota(jnp.int32, (SUB, 128), 0) * (2 * COUNT_FACTOR % 2**32 - (2**32 if 2 * COUNT_FACTOR % 2**32 >= 2**31 else 0))

    def group(i, carry):
        start = pl.multiple_of(i * SUB, SUB)
        mode_terms = row_terms + (first_mode + start) * 2 * COUNT_FACTOR
        for at in range(0, samples, 128):
            first = seeds_ref[:, at:at + 128] * SEED_FACTOR + mode_terms
            high, low = split(normals(first))
            high_ref[pl.ds(start, SUB), at:at + 128] = high
            low_ref[pl.ds(start, SUB), at:at + 128] = low
        return carry

    lax.fori_loop(0, rows // SUB, group, 0)


def draw_kernel(rows, base_ref, seeds_ref, high_ref, low_ref):
    fill_rows(seeds_ref, high_ref, low_ref, base_ref[pl.program_id(0)], rows)


def draw(bases, seeds, rows):
    units = bases.shape[0]
    samples = seeds.shape[1]
    out = jax.ShapeDtypeStruct((units * rows, samples), jnp.bfloat16)
    spec = pl.BlockSpec((rows, samples), lambda i, base: (i, 0))
    return pl.pallas_call(
        functools.partial(draw_kernel, rows),
        grid_spec=pltpu.PrefetchScalarGridSpec(
            num_scalar_prefetch=1,
            grid=(units,),
            in_specs=[pl.BlockSpec((1, samples), lambda i, base: (0, 0))],
            out_specs=[spec, spec],
        ),
        out_shape=[out, out],
        cost_estimate=pl.CostEstimate(flops=DRAW_FLOPS * units * rows * samples, transcendentals=0, bytes_accessed=4 * units * rows * samples),
        name="draw",
    )(bases, seeds)


def scale_kernel(count, at_ref, scales_ref, *refs):
    for source, target in zip(refs[:count], refs[count:]):
        target[...] = scales_ref[...] * source[...]


def scale_pieces(basis, scales, columns, first_row, rows, nodes):
    count = len(columns)
    step = min(128, rows)
    at = jnp.stack([first_row // step, *columns]).astype(jnp.int32)
    out = jax.ShapeDtypeStruct((rows, nodes), jnp.float32)
    return pl.pallas_call(
        functools.partial(scale_kernel, count),
        grid_spec=pltpu.PrefetchScalarGridSpec(
            num_scalar_prefetch=1,
            grid=(rows // step,),
            in_specs=[pl.BlockSpec((step, 1), lambda i, at: (i + at[0], 0))]
            + [pl.BlockSpec((step, nodes), lambda i, at, j=j: (i + at[0], at[j + 1])) for j in range(count)],
            out_specs=[pl.BlockSpec((step, nodes), lambda i, at: (i, 0))] * count,
        ),
        out_shape=[out] * count,
        name="scale_pieces",
    )(at, scales, *[basis] * count)


def dot(a, b):
    return lax.dot_general(a, b, (((0,), (0,)), ((), ())), preferred_element_type=jnp.float32)


def contract_kernel(count, rows, first, last, *refs):
    pieces, refs = refs[:2 * count], refs[2 * count:]
    high_ref, low_ref, refs = refs[0], refs[1], refs[2:]
    if not first:
        before_ref, refs = refs[0], refs[1:]
    if last:
        mean_ref, own_ref, other_ref, sum_ref, basis_high, basis_low, total_ref = refs
    else:
        total_ref, basis_high, basis_low = refs
    step = pl.program_id(0)
    nodes = pieces[0].shape[1]

    @pl.when(step == 0)
    def _():
        for side in range(2):
            start = 0
            for piece in pieces[side * count:(side + 1) * count]:
                size = piece.shape[0]
                high, low = split(piece[...])
                basis_high[start:start + size, side * nodes:(side + 1) * nodes] = high
                basis_low[start:start + size, side * nodes:(side + 1) * nodes] = low
                start += size
        total_ref[...] = jnp.zeros_like(total_ref) if first else before_ref[...]

    at = pl.ds(pl.multiple_of(step * rows, rows), rows)
    high = basis_high[at, :]
    total_ref[...] += dot(high, high_ref[...]) + dot(high, low_ref[...]) + dot(basis_low[at, :], high_ref[...])

    if last:
        @pl.when(step == pl.num_programs(0) - 1)
        def _():
            modulus = jnp.exp(total_ref[...] + mean_ref[...])
            own_ref[...] = modulus[:nodes]
            other_ref[...] = modulus[nodes:]
            sum_ref[...] = jnp.sum(modulus, axis=0, keepdims=True)


def contract(own, other, coeffs, before=None, mean=None):
    count = len(own)
    nodes = own[0].shape[1]
    high, low = coeffs
    modes, samples = high.shape
    rows = min(512, modes)
    whole = lambda *shape: pl.BlockSpec(shape, lambda i: (0, 0))
    spec = pl.BlockSpec((rows, samples), lambda i: (i, 0))
    in_specs = [whole(*piece.shape) for piece in (*own, *other)] + [spec, spec]
    operands = [*own, *other, high, low]
    shape = lambda *dims: jax.ShapeDtypeStruct(dims, jnp.float32)
    scratch = [pltpu.VMEM((modes, 2 * nodes), jnp.bfloat16)] * 2
    if before is not None:
        operands.append(before)
        in_specs.append(whole(2 * nodes, samples))
    if mean is None:
        out_shape = [shape(2 * nodes, samples)]
    else:
        operands.append(mean)
        in_specs.append(whole(2 * nodes, 1))
        out_shape = [shape(nodes, samples), shape(nodes, samples), shape(1, samples)]
        scratch.append(pltpu.VMEM((2 * nodes, samples), jnp.float32))
    return pl.pallas_call(
        functools.partial(contract_kernel, count, rows, before is None, mean is not None),
        grid=(modes // rows,),
        in_specs=in_specs,
        out_specs=[whole(*out.shape) for out in out_shape],
        out_shape=out_shape,
        scratch_shapes=scratch,
        cost_estimate=pl.CostEstimate(flops=12 * modes * nodes * samples, transcendentals=0, bytes_accessed=4 * modes * samples),
        name="contract",
    )(*operands)


def exchange(array, axis, bit):
    return lax.ppermute(array, axis, [(i, i ^ bit) for i in range(lax.axis_size(axis))])


def exchange_both(array, bit):
    cores = lax.axis_size("node")
    size = lax.axis_size("mode") * cores
    pairs = [(i, ((i // cores) ^ bit) * cores + (i % cores ^ 1)) for i in range(size)]
    return lax.ppermute(array, ("mode", "node"), pairs)


def tie(*values):
    return lax.optimization_barrier(values)


def on_device(mode_basis, mode_scales, mean_log, sample_seeds):
    nodes = mean_log.shape[0]
    rows = mode_basis.shape[0]
    shards = lax.axis_size("mode")
    samples = sample_seeds.shape[0] // 2
    mode = lax.axis_index("mode")
    grp = lax.axis_index("grp")
    node = lax.axis_index("node")
    seeds = lax.dynamic_slice_in_dim(sample_seeds, node * samples, samples)[None, :]
    mean = jnp.concatenate([mean_log, exchange(mean_log, "node", 1)])[:, None]
    scales = mode_scales[:, None]
    half = rows // 2

    if shards <= 8:
        near = list(range(shards // 2))
        far = list(range(shards // 2, shards))
        far_out = scale_pieces(mode_basis, scales, [mode ^ k for k in far], grp * half, half, nodes)
        far_in = [exchange(piece, "mode", k) for k, piece in zip(far, far_out)]
        near_out = scale_pieces(mode_basis, scales, [mode ^ k for k in near], 0 * grp, rows, nodes)
        near_in = [near_out[0]] + [exchange(piece, "mode", k) for k, piece in zip(near[1:], near_out[1:])]
        near_bases = [(mode ^ k) * rows + at for k in near for at in (0, half)]
        far_bases = [(mode ^ k) * rows + grp * half for k in far]
        swapped_bases = [(mode ^ k) * rows + (1 - grp) * half for k in far]
        near_drawn = draw(jnp.stack(near_bases).astype(jnp.int32), seeds, half)
        early = len(far) // 2
        near_drawn, seeds, far_in[:early] = tie(near_drawn, seeds, far_in[:early])
        swapped = [exchange(piece, "grp", 1) for piece in far_in[:early]]
        far_drawn = draw(jnp.stack(far_bases + swapped_bases).astype(jnp.int32), seeds, half)
        far_drawn, near_in, far_in[early:] = tie(far_drawn, near_in, far_in[early:])
        swapped += [exchange(piece, "grp", 1) for piece in far_in[early:]]
        groups = [(near_in, near_drawn), (far_in + swapped, far_drawn)]
    else:
        gathered = lax.all_to_all(scales * mode_basis, "mode", split_axis=1, concat_axis=0, tiled=True)
        bases = jnp.stack([k * rows + at + 0 * mode for k in range(shards) for at in (0, half)])
        groups = [([gathered], draw(bases.astype(jnp.int32), seeds, half))]

    total = None
    for index, (pieces, coeffs) in enumerate(groups):
        other = [exchange(piece, "node", 1) for piece in pieces]
        if index < len(groups) - 1:
            total, = contract(pieces, other, coeffs, total)
            later = groups[index + 1]
            total, swapped = tie(total, swapped)
            groups[index + 1] = (later[0][:-len(swapped)] + swapped, later[1])
        else:
            own, lent, sums = contract(pieces, other, coeffs, total, mean)

    returned = exchange(lent, "node", 1)
    modulus = jnp.where(node == 0, jnp.concatenate([own, returned], 1), jnp.concatenate([returned, own], 1))
    sums = sums[0]
    bit = 1
    while 2 * bit < shards:
        one, two, three = (exchange(sums, "mode", bit * k) for k in (1, 2, 3))
        sums = (sums + one) + (two + three)
        bit *= 4
    others = exchange(sums, "node", 1)
    if bit < shards:
        pair = exchange(sums, "mode", bit)
        others = others + exchange_both(sums, bit)
        sums = sums + pair
    totals = jnp.where(node == 0, jnp.concatenate([sums, others]), jnp.concatenate([others, sums]))
    node_count = nodes * shards * lax.axis_size("node")
    return (modulus, totals / node_count)


def solution(mesh):
    return jax.shard_map(
        on_device,
        mesh=mesh,
        in_specs=(P("mode", "node"), P("mode"), P(("node", "mode")), P("grp")),
        out_specs=(P(("node", "mode"), "grp"), P("grp")),
        check_vma=False,
    )
```

```python
import functools

import jax
import jax.numpy as jnp
from jax import lax
from jax.experimental import pallas as pl
from jax.experimental.pallas import tpu as pltpu
from jax.sharding import PartitionSpec as P

SEED_FACTOR = -1640531527
COUNT_FACTOR = 668265261
COS_TERMS = (1.4142134962552295, -6.97885094856384, 5.73946037690727, -1.8835579059862844, 0.31068802752475627)
SUB = 16
DRAW_FLOPS = 8192


def scramble(word):
    word = word ^ lax.shift_right_logical(word, 15)
    word = word * -2048144789
    word = word ^ lax.shift_right_logical(word, 13)
    word = word * -1028477387
    return word ^ lax.shift_right_logical(word, 16)


def normals(first):
    one = scramble(first) & 16777215
    two = scramble(first + COUNT_FACTOR) << 8
    first_unit = one.astype(jnp.float32) * (1.0 / 16777216.0) + (0.5 / 16777216.0)
    turn = two.astype(jnp.float32) * (2.0**-32) + (0.5 / 16777216.0)
    square = jnp.maximum(-2.0 * jnp.log(first_unit), 1e-30)
    radius = square * lax.rsqrt(square)
    arg = turn * turn
    half = jnp.float32(COS_TERMS[-1])
    for term in COS_TERMS[-2::-1]:
        half = half * arg + jnp.float32(term)
    return radius * (half * half - 1.0)


def split(values):
    high = values.astype(jnp.bfloat16)
    return high, (values - high.astype(jnp.float32)).astype(jnp.bfloat16)


def fill_rows(seeds_ref, high_ref, low_ref, first_mode, rows):
    samples = seeds_ref.shape[1]
    row_terms = lax.broadcasted_iota(jnp.int32, (SUB, 128), 0) * (2 * COUNT_FACTOR % 2**32 - (2**32 if 2 * COUNT_FACTOR % 2**32 >= 2**31 else 0))

    def group(i, carry):
        start = pl.multiple_of(i * SUB, SUB)
        mode_terms = row_terms + (first_mode + start) * 2 * COUNT_FACTOR
        for at in range(0, samples, 128):
            first = seeds_ref[:, at:at + 128] * SEED_FACTOR + mode_terms
            high, low = split(normals(first))
            high_ref[pl.ds(start, SUB), at:at + 128] = high
            low_ref[pl.ds(start, SUB), at:at + 128] = low
        return carry

    lax.fori_loop(0, rows // SUB, group, 0)


def draw_kernel(rows, base_ref, seeds_ref, high_ref, low_ref):
    fill_rows(seeds_ref, high_ref, low_ref, base_ref[pl.program_id(0)], rows)


def draw(bases, seeds, rows):
    units = bases.shape[0]
    samples = seeds.shape[1]
    out = jax.ShapeDtypeStruct((units * rows, samples), jnp.bfloat16)
    spec = pl.BlockSpec((rows, samples), lambda i, base: (i, 0))
    return pl.pallas_call(
        functools.partial(draw_kernel, rows),
        grid_spec=pltpu.PrefetchScalarGridSpec(
            num_scalar_prefetch=1,
            grid=(units,),
            in_specs=[pl.BlockSpec((1, samples), lambda i, base: (0, 0))],
            out_specs=[spec, spec],
        ),
        out_shape=[out, out],
        cost_estimate=pl.CostEstimate(flops=DRAW_FLOPS * units * rows * samples, transcendentals=0, bytes_accessed=4 * units * rows * samples),
        name="draw",
    )(bases, seeds)


def scale_kernel(count, at_ref, scales_ref, *refs):
    for source, target in zip(refs[:count], refs[count:]):
        target[...] = scales_ref[...] * source[...]


def scale_pieces(basis, scales, columns, first_row, rows, nodes):
    count = len(columns)
    step = min(128, rows)
    at = jnp.stack([first_row // step, *columns]).astype(jnp.int32)
    out = jax.ShapeDtypeStruct((rows, nodes), jnp.float32)
    return pl.pallas_call(
        functools.partial(scale_kernel, count),
        grid_spec=pltpu.PrefetchScalarGridSpec(
            num_scalar_prefetch=1,
            grid=(rows // step,),
            in_specs=[pl.BlockSpec((step, 1), lambda i, at: (i + at[0], 0))]
            + [pl.BlockSpec((step, nodes), lambda i, at, j=j: (i + at[0], at[j + 1])) for j in range(count)],
            out_specs=[pl.BlockSpec((step, nodes), lambda i, at: (i, 0))] * count,
        ),
        out_shape=[out] * count,
        name="scale_pieces",
    )(at, scales, *[basis] * count)


def dot(a, b):
    return lax.dot_general(a, b, (((0,), (0,)), ((), ())), preferred_element_type=jnp.float32)


def contract_kernel(count, rows, first, last, *refs):
    pieces, refs = refs[:2 * count], refs[2 * count:]
    high_ref, low_ref, refs = refs[0], refs[1], refs[2:]
    if not first:
        before_ref, refs = refs[0], refs[1:]
    if last:
        mean_ref, own_ref, other_ref, sum_ref, basis_high, basis_low, total_ref = refs
    else:
        total_ref, basis_high, basis_low = refs
    step = pl.program_id(0)
    nodes = pieces[0].shape[1]

    @pl.when(step == 0)
    def _():
        for side in range(2):
            start = 0
            for piece in pieces[side * count:(side + 1) * count]:
                size = piece.shape[0]
                high, low = split(piece[...])
                basis_high[start:start + size, side * nodes:(side + 1) * nodes] = high
                basis_low[start:start + size, side * nodes:(side + 1) * nodes] = low
                start += size
        total_ref[...] = jnp.zeros_like(total_ref) if first else before_ref[...]

    at = pl.ds(pl.multiple_of(step * rows, rows), rows)
    high = basis_high[at, :]
    total_ref[...] += dot(high, high_ref[...]) + dot(high, low_ref[...]) + dot(basis_low[at, :], high_ref[...])

    if last:
        @pl.when(step == pl.num_programs(0) - 1)
        def _():
            modulus = jnp.exp(total_ref[...] + mean_ref[...])
            own_ref[...] = modulus[:nodes]
            other_ref[...] = modulus[nodes:]
            sum_ref[...] = jnp.sum(modulus, axis=0, keepdims=True)


def contract(own, other, coeffs, before=None, mean=None):
    count = len(own)
    nodes = own[0].shape[1]
    high, low = coeffs
    modes, samples = high.shape
    rows = min(512, modes)
    whole = lambda *shape: pl.BlockSpec(shape, lambda i: (0, 0))
    spec = pl.BlockSpec((rows, samples), lambda i: (i, 0))
    in_specs = [whole(*piece.shape) for piece in (*own, *other)] + [spec, spec]
    operands = [*own, *other, high, low]
    shape = lambda *dims: jax.ShapeDtypeStruct(dims, jnp.float32)
    scratch = [pltpu.VMEM((modes, 2 * nodes), jnp.bfloat16)] * 2
    if before is not None:
        operands.append(before)
        in_specs.append(whole(2 * nodes, samples))
    if mean is None:
        out_shape = [shape(2 * nodes, samples)]
    else:
        operands.append(mean)
        in_specs.append(whole(2 * nodes, 1))
        out_shape = [shape(nodes, samples), shape(nodes, samples), shape(1, samples)]
        scratch.append(pltpu.VMEM((2 * nodes, samples), jnp.float32))
    return pl.pallas_call(
        functools.partial(contract_kernel, count, rows, before is None, mean is not None),
        grid=(modes // rows,),
        in_specs=in_specs,
        out_specs=[whole(*out.shape) for out in out_shape],
        out_shape=out_shape,
        scratch_shapes=scratch,
        cost_estimate=pl.CostEstimate(flops=12 * modes * nodes * samples, transcendentals=0, bytes_accessed=4 * modes * samples),
        name="contract",
    )(*operands)


def exchange(array, axis, bit):
    return lax.ppermute(array, axis, [(i, i ^ bit) for i in range(lax.axis_size(axis))])


def exchange_both(array, bit):
    cores = lax.axis_size("node")
    size = lax.axis_size("mode") * cores
    pairs = [(i, ((i // cores) ^ bit) * cores + (i % cores ^ 1)) for i in range(size)]
    return lax.ppermute(array, ("mode", "node"), pairs)


def tie(*values):
    return lax.optimization_barrier(values)


def on_device(mode_basis, mode_scales, mean_log, sample_seeds):
    nodes = mean_log.shape[0]
    rows = mode_basis.shape[0]
    shards = lax.axis_size("mode")
    samples = sample_seeds.shape[0] // 2
    mode = lax.axis_index("mode")
    grp = lax.axis_index("grp")
    node = lax.axis_index("node")
    seeds = lax.dynamic_slice_in_dim(sample_seeds, node * samples, samples)[None, :]
    mean = jnp.concatenate([mean_log, exchange(mean_log, "node", 1)])[:, None]
    scales = mode_scales[:, None]
    half = rows // 2

    if shards <= 8:
        near = list(range(shards // 2))
        far = list(range(shards // 2, shards))
        far_out = scale_pieces(mode_basis, scales, [mode ^ k for k in far], grp * half, half, nodes)
        far_in = [exchange(piece, "mode", k) for k, piece in zip(far, far_out)]
        near_out = scale_pieces(mode_basis, scales, [mode ^ k for k in near], 0 * grp, rows, nodes)
        near_in = [near_out[0]] + [exchange(piece, "mode", k) for k, piece in zip(near[1:], near_out[1:])]
        near_bases = [(mode ^ k) * rows + at for k in near for at in (0, half)]
        far_bases = [(mode ^ k) * rows + grp * half for k in far]
        swapped_bases = [(mode ^ k) * rows + (1 - grp) * half for k in far]
        near_drawn = draw(jnp.stack(near_bases).astype(jnp.int32), seeds, half)
        early = len(far) // 2
        near_drawn, seeds, far_in[:early] = tie(near_drawn, seeds, far_in[:early])
        swapped = [exchange(piece, "grp", 1) for piece in far_in[:early]]
        far_drawn = draw(jnp.stack(far_bases).astype(jnp.int32), seeds, half)
        far_drawn, seeds, far_in[early:] = tie(far_drawn, seeds, far_in[early:])
        swapped += [exchange(piece, "grp", 1) for piece in far_in[early:]]
        swapped_drawn = draw(jnp.stack(swapped_bases).astype(jnp.int32), seeds, half)
        swapped_drawn, near_in, far_in = tie(swapped_drawn, near_in, far_in)
        groups = [(near_in, near_drawn), (far_in, far_drawn), (swapped, swapped_drawn)]
    else:
        gathered = lax.all_to_all(scales * mode_basis, "mode", split_axis=1, concat_axis=0, tiled=True)
        bases = jnp.stack([k * rows + at + 0 * mode for k in range(shards) for at in (0, half)])
        groups = [([gathered], draw(bases.astype(jnp.int32), seeds, half))]

    total = None
    for index, (pieces, coeffs) in enumerate(groups):
        other = [exchange(piece, "node", 1) for piece in pieces]
        if index < len(groups) - 1:
            total, = contract(pieces, other, coeffs, total)
            if index == 0:
                total, swapped = tie(total, swapped)
                groups[-1] = (swapped, swapped_drawn)
        else:
            own, lent, sums = contract(pieces, other, coeffs, total, mean)

    returned = exchange(lent, "node", 1)
    modulus = jnp.where(node == 0, jnp.concatenate([own, returned], 1), jnp.concatenate([returned, own], 1))
    sums = sums[0]
    bit = 1
    while 2 * bit < shards:
        one, two, three = (exchange(sums, "mode", bit * k) for k in (1, 2, 3))
        sums = (sums + one) + (two + three)
        bit *= 4
    others = exchange(sums, "node", 1)
    if bit < shards:
        pair = exchange(sums, "mode", bit)
        others = others + exchange_both(sums, bit)
        sums = sums + pair
    totals = jnp.where(node == 0, jnp.concatenate([sums, others]), jnp.concatenate([others, sums]))
    node_count = nodes * shards * lax.axis_size("node")
    return (modulus, totals / node_count)


def solution(mesh):
    return jax.shard_map(
        on_device,
        mesh=mesh,
        in_specs=(P("mode", "node"), P("mode"), P(("node", "mode")), P("grp")),
        out_specs=(P(("node", "mode"), "grp"), P("grp")),
        check_vma=False,
    )
```
